8 devices in a mesh: replica: 4 (over z, y, x), data: 2 (over core).
Axes of the slice: x: 2, y: 2, z: 1, core: 2. Of those that a mesh axis runs over, the one named last changes fastest.
Arguments:
- img_x: bfloat16 [32768, 1280], P(('replica', 'data'))
- txt_x: bfloat16 [32768, 1024], P(('replica', 'data'))
- w_img: bfloat16 [1280, 1024], replicated
- w_txt: bfloat16 [1024, 1024], replicated
- log_temp: float32 [1], replicated
- logit_bias: float32 [1], replicated
Outputs:
- output 1: float32 [1], replicated
- output 2: float32 [1], replicated
- output 3: float32 [1], replicated
- output 4: float32 [1280, 1024], replicated
- output 5: float32 [1024, 1024], replicated
All inputs are finite; a program needn't handle non-finite values.
Results may differ from the reference program's by a relative error of at most 0.001.
Values are sent between devices in bfloat16 or wider.
A program may use at most 1 GiB of HBM per device.

```python
import math
import jax
import jax.numpy as jnp
from jax import lax

LOCAL_BATCH = 4096
NUM_DEVICES = 8
IMG_FEAT = 1280
TXT_FEAT = 1024
EMBED_DIM = 1024
LATENT_RANK = 8

GLOBAL_BATCH = LOCAL_BATCH * NUM_DEVICES


def setup_inputs(seed: int = 0) -> dict:
    key_list = jax.random.split(jax.random.key(seed), 12)
    latent = jax.random.normal(key_list[0], (NUM_DEVICES, LOCAL_BATCH, LATENT_RANK), jnp.float32)
    dev_mean = jax.random.normal(key_list[1], (NUM_DEVICES, 1, LATENT_RANK), jnp.float32)
    latent = (latent + 0.8 * dev_mean).reshape(GLOBAL_BATCH, LATENT_RANK)
    mix_img = jax.random.normal(key_list[2], (LATENT_RANK, IMG_FEAT), jnp.float32) * LATENT_RANK ** -0.5
    mix_txt = jax.random.normal(key_list[3], (LATENT_RANK, TXT_FEAT), jnp.float32) * LATENT_RANK ** -0.5
    shared = jax.random.normal(key_list[4], (LATENT_RANK, EMBED_DIM), jnp.float32)
    img_x = 0.7 * (jnp.dot(latent, mix_img) + jax.random.normal(key_list[5], (GLOBAL_BATCH, IMG_FEAT), jnp.float32))
    txt_x = 0.7 * (jnp.dot(latent, mix_txt) + jax.random.normal(key_list[6], (GLOBAL_BATCH, TXT_FEAT), jnp.float32))
    w_img = jnp.dot(mix_img.T, shared) * (LATENT_RANK ** 0.5 / IMG_FEAT) + jax.random.normal(key_list[7], (IMG_FEAT, EMBED_DIM), jnp.float32) * IMG_FEAT ** -0.5
    w_txt = jnp.dot(mix_txt.T, shared) * (LATENT_RANK ** 0.5 / TXT_FEAT) + jax.random.normal(key_list[8], (TXT_FEAT, EMBED_DIM), jnp.float32) * TXT_FEAT ** -0.5
    log_temp = math.log(4.0) + jax.random.uniform(key_list[9], (1,), jnp.float32, -0.3, 0.3)
    logit_bias = -math.log(GLOBAL_BATCH) + jax.random.uniform(key_list[10], (1,), jnp.float32, -0.5, 0.5)
    return {"img_x": img_x.astype(jnp.bfloat16), "txt_x": txt_x.astype(jnp.bfloat16), "w_img": w_img.astype(jnp.bfloat16), "w_txt": w_txt.astype(jnp.bfloat16), "log_temp": log_temp.astype(jnp.float32), "logit_bias": logit_bias.astype(jnp.float32)}


def normalize(raw):
    return raw * lax.rsqrt(jnp.sum(raw * raw, axis=-1, keepdims=True))


def reference(img_x, txt_x, w_img, w_txt, log_temp, logit_bias):
    img_raw = jnp.dot(img_x, w_img, preferred_element_type=jnp.float32)
    txt_raw = jnp.dot(txt_x, w_txt, preferred_element_type=jnp.float32)
    img_unit, img_pull = jax.vjp(normalize, img_raw)
    txt_unit, txt_pull = jax.vjp(normalize, txt_raw)
    img_emb = img_unit.astype(jnp.bfloat16)
    txt_emb = txt_unit.astype(jnp.bfloat16)
    temp_scale = jnp.exp(log_temp[0])
    bias_val = logit_bias[0]
    col_ids = jnp.arange(GLOBAL_BATCH)[None, :]
    row_ids = jnp.arange(LOCAL_BATCH)[:, None]

    def block_step(state_in, block_in):
        d_txt_acc, loss_acc, temp_acc, bias_acc = state_in
        img_blk, blk_idx = block_in
        sim_tile = jnp.dot(img_blk, txt_emb.T, preferred_element_type=jnp.float32)
        logits = temp_scale * sim_tile + bias_val
        labels = jnp.where(col_ids == row_ids + blk_idx * LOCAL_BATCH, 1.0, -1.0)
        loss_part = -jnp.sum(jax.nn.log_sigmoid(labels * logits))
        grad_tile = -labels * jax.nn.sigmoid(-labels * logits) / GLOBAL_BATCH
        grad_b = grad_tile.astype(jnp.bfloat16)
        d_img_blk = temp_scale * jnp.dot(grad_b, txt_emb, preferred_element_type=jnp.float32)
        d_txt_acc = d_txt_acc + jnp.dot(grad_b.T, img_blk, preferred_element_type=jnp.float32)
        new_state = (d_txt_acc, loss_acc + loss_part, temp_acc + jnp.sum(grad_tile * sim_tile), bias_acc + jnp.sum(grad_tile))
        return new_state, d_img_blk

    init_state = (jnp.zeros((GLOBAL_BATCH, EMBED_DIM), jnp.float32), jnp.zeros((), jnp.float32), jnp.zeros((), jnp.float32), jnp.zeros((), jnp.float32))
    img_blocks = img_emb.reshape(NUM_DEVICES, LOCAL_BATCH, EMBED_DIM)
    final_state, d_img_blocks = lax.scan(block_step, init_state, (img_blocks, jnp.arange(NUM_DEVICES)))
    d_txt_acc, loss_sum, temp_sum, bias_sum = final_state
    d_img = d_img_blocks.reshape(GLOBAL_BATCH, EMBED_DIM)
    d_txt = temp_scale * d_txt_acc
    d_img_raw = img_pull(d_img)[0].astype(jnp.bfloat16)
    d_txt_raw = txt_pull(d_txt)[0].astype(jnp.bfloat16)
    d_w_img = jnp.dot(img_x.T, d_img_raw, preferred_element_type=jnp.float32)
    d_w_txt = jnp.dot(txt_x.T, d_txt_raw, preferred_element_type=jnp.float32)
    loss_out = jnp.reshape(loss_sum / GLOBAL_BATCH, (1,))
    d_log_temp = jnp.reshape(temp_scale * temp_sum, (1,))
    d_logit_bias = jnp.reshape(bias_sum, (1,))
    return (loss_out, d_log_temp, d_logit_bias, d_w_img, d_w_txt)
```

```python
import functools
import jax
import jax.numpy as jnp
from jax import lax
from jax.experimental import pallas as pl
from jax.experimental.pallas import tpu as pltpu
from jax.sharding import PartitionSpec as P


LOG2E = 1.4426950408889634
LN2 = 0.6931471805599453
BM, BN = 512, 512
PIECES, SHIFT = 16, 6


def embed_kernel(x_ref, w_ref, emb_ref, raw_ref):
    raw = jnp.dot(x_ref[...], w_ref[...], preferred_element_type=jnp.float32)
    raw_ref[...] = raw
    emb_ref[...] = (raw * lax.rsqrt(jnp.sum(raw * raw, axis=-1, keepdims=True))).astype(jnp.bfloat16)


def embed_call(feat_x, w_proj):
    rows, feat = feat_x.shape
    dim = w_proj.shape[1]
    out_spec = pl.BlockSpec((BN, dim), lambda j: (j, 0))
    return pl.pallas_call(
        embed_kernel,
        grid=(rows // BN,),
        in_specs=[pl.BlockSpec((BN, feat), lambda j: (j, 0)), pl.BlockSpec((feat, dim), lambda j: (0, 0))],
        out_specs=[out_spec, out_spec],
        out_shape=[jax.ShapeDtypeStruct((rows, dim), jnp.bfloat16), jax.ShapeDtypeStruct((rows, dim), jnp.float32)],
        compiler_params=pltpu.CompilerParams(vmem_limit_bytes=40 * 2**20),
        cost_estimate=pl.CostEstimate(flops=2 * rows * feat * dim, bytes_accessed=2 * rows * feat + 6 * rows * dim, transcendentals=0),
        name="embed",
    )(feat_x, w_proj)


def weight_kernel(n_full, sc_ref, x_ref, raw_ref, *refs):
    parts, (first_ref, second_ref, out_ref) = refs[:n_full], refs[n_full:]
    j = pl.program_id(0)
    raw = raw_ref[...]
    inv = lax.rsqrt(jnp.sum(raw * raw, axis=-1, keepdims=True))
    unit = raw * inv
    total = parts[0][...]
    for p in parts[1:]:
        total = total + p[...]
    far = jnp.where(j < pl.num_programs(0) // 2, first_ref[...], second_ref[...])
    d = sc_ref[0] * (total + far)
    d_raw = inv * (d - unit * jnp.sum(unit * d, axis=-1, keepdims=True))
    part = lax.dot_general(x_ref[...], d_raw.astype(jnp.bfloat16), (((0,), (0,)), ((), ())), preferred_element_type=jnp.float32)

    @pl.when(j == 0)
    def _():
        out_ref[...] = part

    @pl.when(j > 0)
    def _():
        out_ref[...] += part


def weight_call(sc, feat_x, raw, parts, first, second):
    rows, feat = feat_x.shape
    dim = raw.shape[1]
    nh = first.shape[0] // BN
    row_spec = pl.BlockSpec((BN, dim), lambda j: (j, 0))
    return pl.pallas_call(
        functools.partial(weight_kernel, len(parts)),
        grid=(rows // BN,),
        in_specs=[pl.BlockSpec(memory_space=pltpu.SMEM), pl.BlockSpec((BN, feat), lambda j: (j, 0)), row_spec]
        + [row_spec] * len(parts)
        + [pl.BlockSpec((BN, dim), lambda j: (jnp.minimum(j, nh - 1), 0)), pl.BlockSpec((BN, dim), lambda j: (jnp.maximum(j - nh, 0), 0))],
        out_specs=pl.BlockSpec((feat, dim), lambda j: (0, 0)),
        out_shape=jax.ShapeDtypeStruct((feat, dim), jnp.float32),
        compiler_params=pltpu.CompilerParams(vmem_limit_bytes=56 * 2**20),
        cost_estimate=pl.CostEstimate(flops=2 * rows * feat * dim, bytes_accessed=2 * rows * feat + 4 * rows * dim * (len(parts) + 2), transcendentals=0),
        name="weight",
    )(sc, feat_x, raw, *parts, first, second)


def tree(x):
    while x.shape[0] > 1:
        x = x.reshape(x.shape[0] // 2, 2, *x.shape[1:])
        x = x[:, 0] + x[:, 1]
    return x[0]


def pair_kernel(m_rows, diag, has_di, has_dt, *refs):
    refs = list(refs)
    sc_ref, i_ref, t_ref = refs[:3]
    refs = refs[3:]
    di_in = refs.pop(0) if has_di else None
    dt_in = refs.pop(0) if has_dt else None
    st_in, di_out, dt_out, st_out, di_acc, g0, g1, in_sem, out_sem = refs
    j = pl.program_id(0)
    last = pl.num_programs(0) - 1
    bm, bn, dim = BM, BN, di_acc.shape[1]
    steps = m_rows // bm
    pr = bm // PIECES
    scale, bias = sc_ref[0], sc_ref[1]

    def rows(k):
        return pl.ds(pl.multiple_of(k * bm, bm), bm)

    def load_di(k):
        return pltpu.make_async_copy(di_in.at[rows(k)], di_acc.at[rows(k)], in_sem.at[k])

    def store_di(k):
        return pltpu.make_async_copy(di_acc.at[rows(k)], di_out.at[rows(k)], out_sem.at[k])

    @pl.when(j == 0)
    def _():
        st_out[...] = st_in[...]
        if has_di:
            @pl.loop(0, steps)
            def _(k):
                load_di(k).start()
        else:
            @pl.loop(0, steps)
            def _(k):
                di_acc[rows(k), :] = jnp.zeros((bm, dim), jnp.float32)

    if has_dt:
        dt_out[...] = dt_in[...]
    else:
        dt_out[...] = jnp.zeros_like(dt_out)

    def dot_s(k):
        return lax.dot_general(i_ref[rows(k), :], t_ref[...], (((1,), (1,)), ((), ())), preferred_element_type=jnp.float32)

    def make_g(k, s_all, g_buf, marks):
        for r in range(PIECES):
            s = s_all[r * pr:(r + 1) * pr, :].reshape(pr // 8, 8, bn)
            if marks is not None and r >= SHIFT:
                b_vec = bias + jnp.concatenate([marks[r - SHIFT] * 0.0] * (bn // 128), axis=1)[None]
            else:
                b_vec = bias
            w = s * scale + b_vec
            if diag:
                rid = lax.broadcasted_iota(jnp.int32, (pr // 8, 8, bn), 0) * 8 + lax.broadcasted_iota(jnp.int32, (pr // 8, 8, bn), 1) + (k * bm + r * pr)
                cid = lax.broadcasted_iota(jnp.int32, (pr // 8, 8, bn), 2) + j * bn
                pos = rid == cid
                w = jnp.where(pos, -w, w)
            a = w * -LOG2E
            g = 1.0 / (1.0 + jnp.exp2(a))
            e = jnp.exp2(-jnp.abs(a))
            u = 1.0 + e
            if diag:
                g = jnp.where(pos, -g, g)
            g_buf[r * pr:(r + 1) * pr, :] = g.reshape(pr, bn).astype(jnp.bfloat16)
            ug = u.reshape(pr // 32, 4, 8, bn)
            st_out[0] += tree(jnp.maximum(w, 0.0) + (e - (u - 1.0)))
            st_out[1] += tree(jnp.log2((ug[:, 0] * ug[:, 1]) * (ug[:, 2] * ug[:, 3])))
            st_out[2] += tree(g * s)
            st_out[3] += tree(g)

    def use_g(k, g_buf):
        g = g_buf[...]
        di = di_acc[rows(k), :] + jnp.dot(g, t_ref[...], preferred_element_type=jnp.float32)
        di_acc[rows(k), :] = di
        dt = dt_out[...] + lax.dot_general(g, i_ref[rows(k), :], (((0,), (0,)), ((), ())), preferred_element_type=jnp.float32)
        dt_out[...] = dt
        marks = []
        for src in (di, dt):
            for p in range(2):
                for h in range(PIECES // 4):
                    r0 = src.shape[0] * 4 // PIECES * h
                    marks.append(src[r0:r0 + 8, p * (dim // 2):p * (dim // 2) + 128])
        return marks

    def both(ks, g_out, ku, g_in):
        s_all = dot_s(ks)
        marks = use_g(ku, g_in)
        make_g(ks, s_all, g_out, marks)

    def before(k):
        if has_di:
            @pl.when(j == 0)
            def _():
                load_di(k).wait()

    def after(k):
        @pl.when(j == last)
        def _():
            store_di(k).start()

    make_g(0, dot_s(0), g0, None)

    @pl.loop(0, steps // 2 - 1)
    def _(p):
        k = 2 * p
        before(k)
        before(k + 1)
        both(k + 1, g1, k, g0)
        both(k + 2, g0, k + 1, g1)
        after(k)
        after(k + 1)

    before(steps - 2)
    before(steps - 1)
    both(steps - 1, g1, steps - 2, g0)
    use_g(steps - 1, g1)
    after(steps - 2)
    after(steps - 1)

    @pl.when(j == last)
    def _():
        @pl.loop(0, steps)
        def _(k):
            store_di(k).wait()


def pair_call(sc, img, txt, di, dt, stats, diag=False):
    m_rows, dim = img.shape
    n_rows = txt.shape[0]
    any_spec = pl.BlockSpec(memory_space=pl.ANY)
    st_spec = pl.BlockSpec((4, 8, BN), lambda j: (0, 0, 0))
    row_spec = pl.BlockSpec((BN, dim), lambda j: (j, 0))
    in_specs = [pl.BlockSpec(memory_space=pltpu.SMEM), pl.BlockSpec((m_rows, dim), lambda j: (0, 0), pipeline_mode=pl.Buffered(1)), row_spec]
    args = [sc, img, txt]
    aliases = {}
    if di is not None:
        aliases[len(args)] = 0
        args.append(di)
        in_specs.append(any_spec)
    if dt is not None:
        aliases[len(args)] = 1
        args.append(dt)
        in_specs.append(row_spec)
    args.append(stats)
    in_specs.append(st_spec)
    pairs = m_rows * n_rows
    return pl.pallas_call(
        functools.partial(pair_kernel, m_rows, diag, di is not None, dt is not None),
        grid=(n_rows // BN,),
        in_specs=in_specs,
        out_specs=[any_spec, row_spec, st_spec],
        out_shape=[jax.ShapeDtypeStruct((m_rows, dim), jnp.float32), jax.ShapeDtypeStruct((n_rows, dim), jnp.float32), jax.ShapeDtypeStruct((4, 8, BN), jnp.float32)],
        scratch_shapes=[pltpu.VMEM((m_rows, dim), jnp.float32), pltpu.VMEM((BM, BN), jnp.bfloat16), pltpu.VMEM((BM, BN), jnp.bfloat16), pltpu.SemaphoreType.DMA((m_rows // BM,)), pltpu.SemaphoreType.DMA((m_rows // BM,))],
        input_output_aliases=aliases,
        compiler_params=pltpu.CompilerParams(vmem_limit_bytes=56 * 2**20),
        cost_estimate=pl.CostEstimate(flops=6 * pairs * dim, bytes_accessed=8 * n_rows * dim + 10 * m_rows * dim, transcendentals=2 * pairs),
        name="pair_diag" if diag else "pair",
    )(*args)


def solution(mesh):
    dev_count = mesh.shape["replica"] * mesh.shape["data"]
    axes = ("replica", "data")

    def swap(x, bit):
        return lax.ppermute(x, axes, [(k, k ^ bit) for k in range(dev_count)])

    core, chip_x, chip_y = 1, 2, 4

    def run(img_x, txt_x, w_img, w_txt, log_temp, logit_bias):
        local_rows = img_x.shape[0]
        total_rows = local_rows * dev_count
        half = local_rows // 2
        temp_scale = jnp.exp(log_temp[0])
        g_scale = temp_scale / total_rows
        sc = jnp.stack([temp_scale, logit_bias[0]])
        t0, txt_raw = embed_call(txt_x, w_txt)
        i0, img_raw = embed_call(img_x, w_img)
        t1 = swap(t0, core)
        t2a, t2b = swap(t0[:half], chip_y), swap(t0[half:], chip_y)
        i1a, i1b = swap(i0[:half], chip_x), swap(i0[half:], chip_x)
        ta = jnp.concatenate([swap(t2a, core), t2a])
        tb = jnp.concatenate([swap(t2b, core), t2b])
        st = jnp.zeros((4, 8, BN), jnp.float32)

        di0, dt0, st = pair_call(sc, i0, t0, None, None, st, diag=True)
        d1a, dt0, st = pair_call(sc, i1a, t0, None, dt0, st)
        d1a, p1, st = pair_call(sc, i1a, t1, d1a, None, st)
        d1a, pa, st = pair_call(sc, i1a, ta, d1a, None, st)
        d1a, pb, st = pair_call(sc, i1a, tb, d1a, None, st)
        xa = swap(d1a, chip_x)
        di0, pa, st = pair_call(sc, i0, ta, di0, pa, st)
        d1b, pa, st = pair_call(sc, i1b, ta, None, pa, st)
        ca = swap(pa[:half], core)
        d1b, dt0, st = pair_call(sc, i1b, t0, d1b, dt0, st)
        ya = swap(pa[half:] + ca, chip_y)
        d1b, pb, st = pair_call(sc, i1b, tb, d1b, pb, st)
        di0, pb, st = pair_call(sc, i0, tb, di0, pb, st)
        cb = swap(pb[:half], core)
        d1b, p1, st = pair_call(sc, i1b, t1, d1b, p1, st)
        xb = swap(d1b, chip_x)
        yb = swap(pb[half:] + cb, chip_y)
        di0, p1, st = pair_call(sc, i0, t1, di0, p1, st)
        back = swap(p1, core)

        sums = lax.psum(jnp.sum(st, axis=(1, 2)), axes)
        gs = jnp.reshape(g_scale, (1,))
        d_w_img = weight_call(gs, img_x, img_raw, (di0,), xa, xb)
        d_w_txt = weight_call(gs, txt_x, txt_raw, (dt0, back), ya, yb)
        d_w_img, d_w_txt = lax.psum((d_w_img, d_w_txt), axes)
        loss_out = jnp.reshape((sums[0] + LN2 * sums[1]) / total_rows, (1,))
        d_log_temp = jnp.reshape(g_scale * sums[2], (1,))
        d_logit_bias = jnp.reshape(sums[3] / total_rows, (1,))
        return loss_out, d_log_temp, d_logit_bias, d_w_img, d_w_txt

    batch_spec = P(axes, None)
    return jax.shard_map(run, mesh=mesh, in_specs=(batch_spec, batch_spec, P(), P(), P(), P()), out_specs=(P(), P(), P(), P(), P()), check_vma=False)
```
